8 devices in a mesh: dp: 2 (over z, y), cp: 4 (over x, core).
Axes of the slice: x: 2, y: 2, z: 1, core: 2. Of those that a mesh axis runs over, the one named last changes fastest.
Arguments:
- hidden: bfloat16 [24, 1536, 2048], P('dp', 'cp')
- positions: int32 [1536], P('cp')
- w_q: bfloat16 [2048, 2048], replicated
- w_k: bfloat16 [2048, 2048], replicated
- w_v: bfloat16 [2048, 2048], replicated
- w_o: bfloat16 [2048, 2048], replicated
Outputs:
- output 1: bfloat16 [24, 1536, 2048], P('dp', 'cp')
- output 2: float32 [16], replicated
- output 3: bfloat16 [2048, 2048], replicated
- output 4: bfloat16 [2048, 2048], replicated
All inputs are finite; a program needn't handle non-finite values.
Results may differ from the reference program's by a relative error of at most 0.00772671.
Values are sent between devices in bfloat16 or wider.
A program may use at most 1 GiB of HBM per device.

```python
import jax
import jax.numpy as jnp
from jax import lax

BATCH_SIZE = 24
SEQ_LEN = 1536
D_MODEL = 2048
NUM_HEADS = 16
QUERY_BLOCK = 64
HEAD_DIM = 128
TAU_CLIP = 100
ROPE_THETA = 50000


def rope_rotate(tensor, pos_ids):
    half_dim = HEAD_DIM // 2
    inv_freq = jnp.float32(ROPE_THETA) ** (-jnp.arange(half_dim, dtype=jnp.float32) * (2.0 / HEAD_DIM))
    angle = pos_ids.astype(jnp.float32)[:, None] * inv_freq[None, :]
    cos_t = jnp.cos(angle)[:, None, :]
    sin_t = jnp.sin(angle)[:, None, :]
    lead_half = tensor[..., :half_dim]
    tail_half = tensor[..., half_dim:]
    return jnp.concatenate([lead_half * cos_t - tail_half * sin_t, tail_half * cos_t + lead_half * sin_t], axis=-1)


def setup_inputs(seed: int = 0) -> dict:
    root_key = jax.random.key(seed)
    sub_keys = jax.random.split(root_key, 15)
    width = NUM_HEADS * HEAD_DIM
    gaps = jax.random.randint(sub_keys[0], (SEQ_LEN,), 1, 3)
    start_pos = jax.random.randint(sub_keys[1], (), 0, SEQ_LEN // 2 + 1)
    positions = (start_pos + jnp.cumsum(gaps) - 1).astype(jnp.int32)
    spike_row = jax.random.randint(sub_keys[2], (), 0, BATCH_SIZE)
    key_slot = jax.random.randint(sub_keys[3], (), 0, SEQ_LEN // 2)
    query_slot = jax.random.randint(sub_keys[4], (), SEQ_LEN // 2, SEQ_LEN)
    clip_heads = (jax.random.permutation(sub_keys[5], NUM_HEADS) < NUM_HEADS // 2).astype(jnp.float32)
    head_gain = jax.random.uniform(sub_keys[6], (NUM_HEADS,), jnp.float32, 1.0, 1.25)
    dir_query = jax.random.normal(sub_keys[7], (D_MODEL,), jnp.float32)
    dir_query = dir_query / jnp.sqrt(jnp.sum(dir_query * dir_query))
    dir_key = jax.random.normal(sub_keys[8], (D_MODEL,), jnp.float32)
    dir_key = dir_key / jnp.sqrt(jnp.sum(dir_key * dir_key))
    plant_q = jax.random.normal(sub_keys[9], (NUM_HEADS, HEAD_DIM), jnp.float32)
    plant_q = plant_q / jnp.sqrt(jnp.mean(plant_q * plant_q, axis=-1, keepdims=True))
    plant_q = plant_q * (4.0 * head_gain * clip_heads)[:, None] * D_MODEL ** -0.5
    delta = positions[query_slot] - positions[key_slot]
    plant_k = rope_rotate(plant_q[None], delta[None])[0]
    noise_scale = 1.5 * D_MODEL ** -0.5
    w_q = noise_scale * jax.random.normal(sub_keys[10], (D_MODEL, width), jnp.float32) + dir_query[:, None] * plant_q.reshape(width)[None, :]
    w_k = noise_scale * jax.random.normal(sub_keys[11], (D_MODEL, width), jnp.float32) + dir_key[:, None] * plant_k.reshape(width)[None, :]
    w_v = jax.random.normal(sub_keys[12], (D_MODEL, width), jnp.float32) * D_MODEL ** -0.5
    w_o = jax.random.normal(sub_keys[13], (width, D_MODEL), jnp.float32) * width ** -0.5
    hidden = jax.random.normal(sub_keys[14], (BATCH_SIZE, SEQ_LEN, D_MODEL), jnp.float32)
    spike_scale = jnp.sqrt(jnp.float32(D_MODEL))
    hidden = hidden.at[spike_row, query_slot].set(spike_scale * dir_query)
    hidden = hidden.at[spike_row, key_slot].set(spike_scale * dir_key)
    return {
        "hidden": hidden.astype(jnp.bfloat16),
        "positions": positions,
        "w_q": w_q.astype(jnp.bfloat16),
        "w_k": w_k.astype(jnp.bfloat16),
        "w_v": w_v.astype(jnp.bfloat16),
        "w_o": w_o.astype(jnp.bfloat16),
    }


def reference(hidden, positions, w_q, w_k, w_v, w_o):
    score_scale = HEAD_DIM ** -0.5
    n_blocks = SEQ_LEN // QUERY_BLOCK
    pos_blocks = positions.reshape(n_blocks, QUERY_BLOCK)
    head_shape = (SEQ_LEN, NUM_HEADS, HEAD_DIM)

    def one_row(row_in):
        q_all = rope_rotate(jnp.dot(row_in, w_q, preferred_element_type=jnp.float32).reshape(head_shape), positions).astype(jnp.bfloat16)
        k_all = rope_rotate(jnp.dot(row_in, w_k, preferred_element_type=jnp.float32).reshape(head_shape), positions).astype(jnp.bfloat16)
        v_all = jnp.dot(row_in, w_v, preferred_element_type=jnp.float32).astype(jnp.bfloat16).reshape(head_shape)
        k_wide = k_all.astype(jnp.float32)
        v_wide = v_all.astype(jnp.float32)
        q_blocks = q_all.reshape(n_blocks, QUERY_BLOCK, NUM_HEADS, HEAD_DIM)

        def one_block(block_in):
            q_blk, pos_blk = block_in
            scores = jnp.einsum("qhd,khd->hqk", q_blk.astype(jnp.float32), k_wide) * score_scale
            allowed = positions[None, None, :] <= pos_blk[None, :, None]
            scores = jnp.where(allowed, scores, -jnp.inf)
            block_max = jnp.max(scores, axis=(1, 2))
            prob_w = jax.nn.softmax(scores, axis=-1)
            attn_blk = jnp.einsum("hqk,khd->qhd", prob_w, v_wide)
            return attn_blk.astype(jnp.bfloat16), block_max

        attn_blocks, block_maxes = lax.map(one_block, (q_blocks, pos_blocks))
        attn_flat = attn_blocks.reshape(SEQ_LEN, NUM_HEADS * HEAD_DIM)
        row_out = jnp.dot(attn_flat, w_o, preferred_element_type=jnp.float32).astype(jnp.bfloat16)
        return row_out, jnp.max(block_maxes, axis=0)

    attn_out, row_maxes = lax.map(one_row, hidden)
    head_max = jnp.max(row_maxes, axis=0)
    factor = jnp.where(head_max > TAU_CLIP, jnp.sqrt(TAU_CLIP / head_max), 1.0)
    col_factor = jnp.repeat(factor, HEAD_DIM)
    w_q_new = (w_q.astype(jnp.float32) * col_factor[None, :]).astype(jnp.bfloat16)
    w_k_new = (w_k.astype(jnp.float32) * col_factor[None, :]).astype(jnp.bfloat16)
    return attn_out, head_max, w_q_new, w_k_new
```

```python
import functools

import jax
import jax.numpy as jnp
from jax import lax
from jax.experimental import pallas as pl
from jax.experimental.pallas import tpu as pltpu
from jax.sharding import PartitionSpec as P


HEAD_DIM = 128
TAU_CLIP = 100.0
ROPE_THETA = 50000.0
LOG2_E = 1.4426950408889634
VMEM_LIMIT = 60 * 1024 * 1024
COL_BLOCK = 512
PROJ_BLOCK = 256
QUERY_BLOCK = 256
STEP_HEADS = 2


def rope_tables(pos_ids):
    half_dim = HEAD_DIM // 2
    lane = jnp.arange(HEAD_DIM, dtype=jnp.int32)
    freq_at = (lane % half_dim).astype(jnp.float32)
    inv_freq = jnp.float32(ROPE_THETA) ** (-freq_at * (2.0 / HEAD_DIM))
    angle = pos_ids.astype(jnp.float32)[:, None] * inv_freq[None, :]
    sin_t = jnp.sin(angle)
    return jnp.cos(angle), jnp.where(lane[None, :] < half_dim, -sin_t, sin_t)


def rotate(prod, cos_t, sin_t):
    heads = []
    for lo in range(0, prod.shape[1], HEAD_DIM):
        part = prod[:, lo:lo + HEAD_DIM]
        heads.append((part * cos_t + pltpu.roll(part, HEAD_DIM // 2, 1) * sin_t).astype(jnp.bfloat16))
    return jnp.concatenate(heads, axis=1)


def project_kernel(n_copy, lead_ref, tokens_ref, wq_ref, wk_ref, wv_ref, cos_ref, sin_ref, *refs):
    sources, (q_ref, k_ref, v_ref), copies = refs[:n_copy], refs[n_copy:n_copy + 3], refs[n_copy + 3:]
    for source, copy in zip(sources, copies):
        copy[...] = source[...]
    for row in range(q_ref.shape[0]):
        for w_ref, out_ref in ((wq_ref, q_ref), (wk_ref, k_ref), (wv_ref, v_ref)):
            prod = jnp.dot(tokens_ref[row], w_ref[...], preferred_element_type=jnp.float32)
            out_ref[row] = prod.astype(jnp.bfloat16) if w_ref is wv_ref else rotate(prod, cos_ref[...], sin_ref[...])


def project(lead, n_copy, n_rows, tokens, w_q, w_k, w_v, cos_t, sin_t):
    _, piece, d_model = tokens.shape
    width = w_q.shape[1]
    n_steps = width // PROJ_BLOCK
    w_spec = pl.BlockSpec((d_model, PROJ_BLOCK), lambda n, lead: (0, n))
    table_spec = pl.BlockSpec((piece, HEAD_DIM), lambda n, lead: (0, 0))
    out_spec = pl.BlockSpec((n_rows, piece, PROJ_BLOCK), lambda n, lead: (0, 0, n))
    out = jax.ShapeDtypeStruct((n_rows, piece, width), jnp.bfloat16)
    strip = (1, piece // n_steps, d_model)

    def source_spec(at):
        return pl.BlockSpec(strip, lambda n, lead: (lead[at], n, 0))

    return pl.pallas_call(
        functools.partial(project_kernel, n_copy),
        grid_spec=pltpu.PrefetchScalarGridSpec(
            num_scalar_prefetch=1,
            grid=(n_steps,),
            in_specs=[pl.BlockSpec((n_rows, piece, d_model), lambda n, lead: (lead[0], 0, 0)),
                      w_spec, w_spec, w_spec, table_spec, table_spec] + [source_spec(1 + i) for i in range(n_copy)],
            out_specs=[out_spec] * 3 + [pl.BlockSpec(strip, lambda n, lead: (0, n, 0))] * n_copy,
        ),
        out_shape=[out] * 3 + [jax.ShapeDtypeStruct((1, piece, d_model), jnp.bfloat16)] * n_copy,
        compiler_params=pltpu.CompilerParams(vmem_limit_bytes=VMEM_LIMIT),
        cost_estimate=pl.CostEstimate(flops=3 * 2 * n_rows * piece * d_model * width,
                                      bytes_accessed=6 * d_model * width + 8 * n_rows * piece * width,
                                      transcendentals=0),
    )(lead, tokens, w_q, w_k, w_v, cos_t, sin_t, *[tokens] * n_copy)


def row_kernel(n_proj, n_groups, index_ref, *refs):
    tokens, weights, (cos_ref, sin_ref) = refs[0:2], refs[2:5], refs[5:7]
    own, near, wo_ref = refs[7:10], refs[10:13], refs[13]
    out_refs, max_ref = refs[14:18], refs[18]
    far, qkv_scr, attn_scr = refs[-7:-4], refs[-4:-1], refs[-1]
    step = pl.program_id(0)
    piece = own[0].shape[-2]
    seq_n = 4 * piece
    starts = [pl.multiple_of(index_ref[x] * piece, piece) for x in range(4)]

    @pl.when(step < n_proj)
    def _():
        cols = pl.ds(pl.multiple_of(step * PROJ_BLOCK, PROJ_BLOCK), PROJ_BLOCK)
        for which in range(2):
            for kind in range(3):
                prod = jnp.dot(tokens[which][0], weights[kind][...], preferred_element_type=jnp.float32)
                far[kind][which, :, cols] = prod.astype(jnp.bfloat16) if kind == 2 else rotate(prod, cos_ref[which], sin_ref[which])

    @pl.when((step >= n_proj) & (step < n_proj + n_groups))
    def _():
        group = STEP_HEADS * HEAD_DIM
        group_cols = pl.ds(pl.multiple_of((step - n_proj) * group, group), group)
        for kind, scr in enumerate(qkv_scr):
            blocks = (own[kind][0], near[kind][0], far[kind][0, :, group_cols], far[kind][1, :, group_cols])
            for start, block in zip(starts, blocks):
                scr[pl.ds(start, piece), :] = block
        q_scr, k_scr, v_scr = qkv_scr
        diagonal = (lax.broadcasted_iota(jnp.int32, (QUERY_BLOCK, QUERY_BLOCK), 0)
                    >= lax.broadcasted_iota(jnp.int32, (QUERY_BLOCK, QUERY_BLOCK), 1))

        def logits(head, blk):
            lo, hi = blk * QUERY_BLOCK, (blk + 1) * QUERY_BLOCK
            cols = slice(head * HEAD_DIM, (head + 1) * HEAD_DIM)
            q_blk = q_scr[lo:hi, cols]
            dims = (((1,), (1,)), ((), ()))
            diag = lax.dot_general(q_blk, k_scr[lo:hi, cols], dims, preferred_element_type=jnp.float32)
            parts = [jnp.where(diagonal, diag, -jnp.inf)]
            if blk:
                parts.insert(0, lax.dot_general(q_blk, k_scr[:lo, cols], dims, preferred_element_type=jnp.float32))
            return parts

        items = [(head, blk) for head in range(STEP_HEADS) for blk in range(seq_n // QUERY_BLOCK)]
        tops = [jnp.full((1, 1), -jnp.inf, jnp.float32) for _ in range(STEP_HEADS)]
        ahead = logits(*items[0])
        for at, (head, blk) in enumerate(items):
            parts = ahead
            if at + 1 < len(items):
                ahead = logits(*items[at + 1])
            lo, hi = blk * QUERY_BLOCK, (blk + 1) * QUERY_BLOCK
            cols = slice(head * HEAD_DIM, (head + 1) * HEAD_DIM)
            row_max = functools.reduce(jnp.maximum, [jnp.max(s, axis=1, keepdims=True) for s in parts])
            probs = [jnp.exp2((s - row_max) * (HEAD_DIM ** -0.5 * LOG2_E)) for s in parts]
            row_sum = functools.reduce(jnp.add, [jnp.sum(p, axis=1, keepdims=True) for p in probs])
            spans = [(lo, hi)] if blk == 0 else [(0, lo), (lo, hi)]
            acc = functools.reduce(jnp.add, [
                jnp.dot(p.astype(jnp.bfloat16), v_scr[a:b, cols], preferred_element_type=jnp.float32)
                for p, (a, b) in zip(probs, spans)])
            out = (acc / row_sum).astype(jnp.bfloat16)
            out_cols = pl.ds(pl.multiple_of((step - n_proj) * group + head * HEAD_DIM, HEAD_DIM), HEAD_DIM)
            attn_scr[lo:hi, out_cols] = out
            tops[head] = jnp.maximum(tops[head], jnp.max(row_max, axis=0, keepdims=True))
        for head in range(STEP_HEADS):
            max_ref[head] = jnp.broadcast_to(tops[head] * (HEAD_DIM ** -0.5), max_ref.shape[1:])

    @pl.when(step >= n_proj + n_groups)
    def _():
        for start, o_ref in zip(starts, out_refs):
            o_ref[...] = jnp.dot(attn_scr[pl.ds(start, piece), :], wo_ref[...],
                                 preferred_element_type=jnp.float32).astype(jnp.bfloat16)


def row_block(index, tokens, weights, cos_t, sin_t, own, near, w_o, spare=None):
    _, piece, width = own[0].shape
    n_heads = width // HEAD_DIM
    d_model = w_o.shape[1]
    seq_n = 4 * piece
    n_proj, n_out = width // PROJ_BLOCK, d_model // COL_BLOCK
    n_groups, group = n_heads // STEP_HEADS, STEP_HEADS * HEAD_DIM

    def group_at(s):
        return jnp.clip(s - n_proj, 0, n_groups - 1)

    def out_at(s):
        return jnp.maximum(s - n_proj - n_groups, 0)

    token_spec = pl.BlockSpec((1, piece, d_model), lambda s, ix: (0, 0, 0))
    w_spec = pl.BlockSpec((d_model, PROJ_BLOCK), lambda s, ix: (0, jnp.minimum(s, n_proj - 1)))
    table_spec = pl.BlockSpec((2, piece, HEAD_DIM), lambda s, ix: (0, 0, 0))
    near_spec = pl.BlockSpec((1, piece, group), lambda s, ix: (ix[4], 0, group_at(s)))
    out_spec = pl.BlockSpec((piece, COL_BLOCK), lambda s, ix: (0, out_at(s)))
    out = jax.ShapeDtypeStruct((piece, d_model), jnp.bfloat16)
    extra = [] if spare is None else [jax.ShapeDtypeStruct(spare, jnp.bfloat16)]
    return pl.pallas_call(
        functools.partial(row_kernel, n_proj, n_groups),
        grid_spec=pltpu.PrefetchScalarGridSpec(
            num_scalar_prefetch=1,
            grid=(n_proj + n_groups + n_out,),
            in_specs=[token_spec] * 2 + [w_spec] * 3 + [table_spec] * 2 + [near_spec] * 6
            + [pl.BlockSpec((width, COL_BLOCK), lambda s, ix: (0, out_at(s)))],
            out_specs=[out_spec] * 4 + [pl.BlockSpec((STEP_HEADS, 8, 128), lambda s, ix: (group_at(s), 0, 0))]
            + [pl.BlockSpec(memory_space=pltpu.HBM)] * len(extra),
            scratch_shapes=[pltpu.VMEM((2, piece, width), jnp.bfloat16)] * 3
            + [pltpu.VMEM((seq_n, group), jnp.bfloat16)] * 3 + [pltpu.VMEM((seq_n, width), jnp.bfloat16)],
        ),
        out_shape=[out] * 4 + [jax.ShapeDtypeStruct((n_heads, 8, 128), jnp.float32)] + extra,
        compiler_params=pltpu.CompilerParams(vmem_limit_bytes=VMEM_LIMIT),
        cost_estimate=pl.CostEstimate(flops=5 * seq_n * width * d_model + 4 * seq_n * seq_n * width,
                                      bytes_accessed=8 * width * d_model + 8 * seq_n * width,
                                      transcendentals=seq_n * seq_n * n_heads // 2),
    )(index, *tokens, *weights, cos_t, sin_t, *own, *near, w_o)


def place_kernel(n_chunks, rows_ref, whole_ref, *refs):
    step = pl.program_id(0)
    for at, chunk_ref in enumerate(refs[:n_chunks]):
        @pl.when(step // 2 == at)
        def _():
            @pl.loop(0, chunk_ref.shape[0] // 32)
            def _(part):
                rows = pl.ds(pl.multiple_of(part * 32, 32), 32)
                refs[-1][0, rows, :] = chunk_ref[rows, :]


def place(whole, chunks, rows):
    piece, d_model = chunks[0].shape
    strip = piece // 2

    def chunk_spec(at):
        return pl.BlockSpec((strip, d_model), lambda i, rows: (jnp.clip(i - 2 * at, 0, 1), 0))

    return pl.pallas_call(
        functools.partial(place_kernel, len(chunks)),
        grid_spec=pltpu.PrefetchScalarGridSpec(
            num_scalar_prefetch=1,
            grid=(2 * len(chunks),),
            in_specs=[pl.BlockSpec(memory_space=pltpu.HBM)] + [chunk_spec(at) for at in range(len(chunks))],
            out_specs=pl.BlockSpec((1, strip, d_model), lambda i, rows: (rows[i // 2], i % 2, 0)),
        ),
        out_shape=jax.ShapeDtypeStruct(whole.shape, whole.dtype),
        input_output_aliases={1: 0},
        cost_estimate=pl.CostEstimate(flops=len(chunks) * piece * d_model, bytes_accessed=4 * len(chunks) * piece * d_model,
                                      transcendentals=0),
    )(jnp.stack(rows), whole, *chunks)


def clip_weights(head_max, w_q, w_k):
    factor = jnp.where(head_max > TAU_CLIP, jnp.sqrt(TAU_CLIP / head_max), 1.0)
    col_factor = jnp.repeat(factor, HEAD_DIM)[None, :]
    return (w_q.astype(jnp.float32) * col_factor).astype(jnp.bfloat16), (w_k.astype(jnp.float32) * col_factor).astype(jnp.bfloat16)


def solution(mesh):
    cp_size = mesh.shape["cp"]
    pairs = {x: [(i, i ^ x) for i in range(cp_size)] for x in range(1, cp_size)}

    def layer(hidden, pos_ids, w_q, w_k, w_v, w_o):
        rank = lax.axis_index("cp")
        batch_n, piece, d_model = hidden.shape
        n_rows = batch_n // cp_size
        peer = [rank ^ x for x in range(cp_size)]
        weights = (w_q, w_k, w_v)
        zero = jnp.zeros((1,), jnp.int32)

        def swap(value, x):
            return lax.ppermute(value, "cp", pairs[x])

        def slab(source, x, row, count):
            return lax.dynamic_slice(source, (peer[x] * n_rows + row, 0, 0), (count, piece, d_model))

        first = [slab(hidden, x, 0, 1) for x in (2, 3)]
        hidden_b, pos_b, _ = lax.optimization_barrier((hidden, pos_ids, first))
        near_in = swap(slab(hidden_b, 1, 0, n_rows), 1)
        pos_near, *pos_far = [swap(pos_b, x) for x in range(1, cp_size)]
        later = [(row, x) for row in range(1, n_rows) for x in (2, 3)]
        lead = jnp.stack([peer[0]] + [peer[x] * n_rows + row for row, x in later])
        *own, a, b, c, d = project(lead, len(later), n_rows, hidden, *weights, *rope_tables(pos_ids))
        far_slabs = [first, [a, b], [c, d]]
        far = [[swap(value, x) for value, x in zip(slabs, (2, 3))] for slabs in far_slabs]

        near_in, pos_near, _ = lax.optimization_barrier((near_in, pos_near, own[0]))
        near = project(zero, 0, n_rows, near_in, *weights, *rope_tables(pos_near))

        pos_far, _ = lax.optimization_barrier((pos_far, near[0]))
        far_tables = [t.reshape(2, piece, HEAD_DIM) for t in rope_tables(jnp.concatenate(pos_far))]
        outs, maxes = [], []
        before = near[0]
        for row in range(n_rows):
            last = row == n_rows - 1
            tokens, _ = lax.optimization_barrier((far[row], before))
            got = row_block(jnp.stack([*peer, jnp.int32(row)]), tokens, weights, *far_tables, own, near, w_o, hidden.shape if last else None)
            before = got[4]
            maxes.append(got[4][:, 0, 0])
            outs.append([got[0]] + [swap(got[x], x) for x in range(1, cp_size)])
        out = got[5]
        top = functools.reduce(jnp.maximum, maxes)
        top = jnp.maximum(top, lax.ppermute(top, "dp", [(0, 1), (1, 0)]))
        top = jnp.maximum(top, swap(top, 1))
        head_max = jnp.maximum(top, swap(top, 2))
        out, _ = lax.optimization_barrier((out, top))
        early = [(row, x) for row in range(n_rows - 1) for x in range(cp_size)]
        out = place(out, [outs[row][x] for row, x in early], [peer[x] * n_rows + row for row, x in early])
        for x in range(cp_size):
            out = lax.dynamic_update_slice(out, outs[-1][x][None], (peer[x] * n_rows + n_rows - 1, 0, 0))
        w_q_new, w_k_new = clip_weights(head_max, w_q, w_k)
        return out, head_max, w_q_new, w_k_new

    return jax.shard_map(
        layer,
        mesh=mesh,
        in_specs=(P("dp", "cp", None), P("cp"), P(None, None), P(None, None), P(None, None), P(None, None)),
        out_specs=(P("dp", "cp", None), P(None), P(None, None), P(None, None)),
        check_vma=False,
    )
```
